32 devices in a mesh: dom: 32 (over z, y, x, core).
Axes of the slice: x: 2, y: 2, z: 4, core: 2. Of those that a mesh axis runs over, the one named last changes fastest.
Arguments:
- features: bfloat16 [8192, 512], P('dom'), may hold values from -6 to 6
- w_one: bfloat16 [9, 512, 512], replicated, may hold values from -0.25 to 0.25
- w_two: bfloat16 [8, 512, 349], replicated, may hold values from -0.25 to 0.25
- self_two: bfloat16 [512, 349], replicated, may hold values from -80 to 80
- edge_src: int32 [8, 64, 256], P(None, 'dom'), may hold values from 0 to 511, as said below
- edge_dst: int32 [8, 64, 256], P(None, 'dom'), may hold values from -1 to 127, as said below
- send_rows: int32 [32, 32, 8], P('dom'), may hold values from 0 to 255
- send_count: int32 [32, 32], P('dom'), may hold values from 1 to 8, as said below
- labels: int32 [8192], P('dom'), may hold values from -1 to 348
Outputs:
- logits: float32 [8192, 349], P('dom')
- loss: float32 [], replicated
- grad_one: float32 [4608, 512], P('dom')
- grad_two: float32 [4608, 349], P('dom')
The draws below stay inside these ranges and needn't reach their ends.
Inputs may be any that keep to these rules, and one draw needn't show every extreme that they name: `send_rows`: entry [p, q, s] is a row of partition p's own nodes, rows may repeat. `send_count`: entry [p, q] counts the live slots p sends to q; every row reaches 8 at some q. `edge_src`: index into the destination partition's table: its 256 own rows, then 8 slots from each partition in order. `edge_dst`: -1 marks an empty edge slot.
All inputs are finite; a program needn't handle non-finite values.
Results may differ from the reference program's by a relative error of at most 0.0085.
The reference program's roundings to bfloat16 on the way count: a program that leaves them out, or rounds other values in their place, can miss the bound.
Values may be sent and summed in bfloat16 or wider, within the bound.
A program may use at most 128 MiB of HBM per device.

```python
import jax
import jax.numpy as jnp
from jax import lax

D = 512
CLASSES = 349
RELATIONS = 8
NODES_DEV = 256
SLOTS = 8
EDGES_BLOCK = 256
NODES = 8192
N_DOM = 32


def slot_counts(key):
    base_key = jax.random.fold_in(key, 7)
    limits = jax.random.randint(jax.random.fold_in(base_key, 1), (N_DOM, 1), 1, SLOTS + 1)
    counts = jax.random.randint(jax.random.fold_in(base_key, 2), (N_DOM, N_DOM), 1, SLOTS + 1)
    counts = jnp.minimum(counts, limits)
    full_peer = jax.random.randint(jax.random.fold_in(base_key, 3), (N_DOM, 1), 0, N_DOM)
    peer_ids = jnp.arange(N_DOM, dtype=jnp.int32)[None, :]
    return jnp.where(peer_ids == full_peer, SLOTS, counts).astype(jnp.int32)


def edge_tables(key):
    counts = slot_counts(key)
    base_key = jax.random.fold_in(key, 11)
    blocks = NODES // 128
    edge_shape = (RELATIONS, blocks, EDGES_BLOCK)
    owner_dev = (jnp.arange(blocks, dtype=jnp.int32) // (NODES_DEV // 128))[None, :, None] * jnp.ones(edge_shape, jnp.int32)
    live_level = jax.random.randint(jax.random.fold_in(base_key, 1), (N_DOM,), 4, 11)
    live_edge = jax.random.randint(jax.random.fold_in(base_key, 2), edge_shape, 0, 10) < live_level[owner_dev]
    targets = jnp.where(live_edge, jax.random.randint(jax.random.fold_in(base_key, 3), edge_shape, 0, 128), -1)
    remote = jax.random.randint(jax.random.fold_in(base_key, 4), edge_shape, 0, 2) == 1
    peer_pick = jax.random.randint(jax.random.fold_in(base_key, 5), edge_shape, 0, N_DOM)
    slot_limit = counts[peer_pick, owner_dev]
    slot_pick = jax.random.randint(jax.random.fold_in(base_key, 6), edge_shape, 0, 1 << 20) % slot_limit
    remote_row = NODES_DEV + peer_pick * SLOTS + slot_pick
    local_row = jax.random.randint(jax.random.fold_in(base_key, 7), edge_shape, 0, NODES_DEV)
    sources = jnp.where(remote, remote_row, local_row)
    return (sources.astype(jnp.int32), targets.astype(jnp.int32))


def draw_send_count(key, part):
    return slot_counts(key)


def draw_edge_src(key, part):
    return edge_tables(key)[0]


def draw_edge_dst(key, part):
    return edge_tables(key)[1]


def draw_labels(key, part):
    base_key = jax.random.fold_in(key, 23)
    device_of = jnp.arange(NODES, dtype=jnp.int32) // NODES_DEV
    chance = jax.random.randint(jax.random.fold_in(base_key, 1), (NODES,), 0, 1000)
    labelled = chance < 250 + 500 * device_of // max(N_DOM - 1, 1)
    classes = jax.random.randint(jax.random.fold_in(base_key, 2), (NODES,), 0, CLASSES)
    return jnp.where(labelled, classes, -1).astype(jnp.int32)


def draw_self_two(key, part):
    base_key = jax.random.fold_in(key, 31)
    values = jax.random.normal(jax.random.fold_in(base_key, 1), (D, CLASSES), jnp.float32) * D ** (-0.5)
    return jnp.clip(values, -80.0, 80.0).astype(jnp.bfloat16)


def set_ends(drawn, own_key, least, top_value):
    spot = [jax.random.randint(jax.random.fold_in(own_key, axis), (), 0, length) for axis, length in enumerate(drawn.shape)]
    widest = drawn.shape.index(max(drawn.shape))
    neighbour = spot[:widest] + [(spot[widest] + 1) % drawn.shape[widest]] + spot[widest + 1:]
    return drawn.at[tuple(spot)].set(least).at[tuple(neighbour)].set(top_value)


def level_of(rng, shape, shards, least, high):
    def one(position, shards_of):
        heights = jax.random.uniform(jax.random.fold_in(jax.random.fold_in(rng, 6), position), (shards_of,), jnp.float32, least / len(shards), high / len(shards))
        return jnp.repeat(jnp.exp(heights), shape[position] // shards_of).reshape((-1,) + (1,) * (len(shape) - position - 1))

    level = one(*shards[0])
    for cut in shards[1:]:
        level = level * one(*cut)
    return level


def scatter_about(key, shape, scale, bound, cuts=(), kind=jnp.bfloat16):
    factor_of = level_of(key, shape, cuts, -0.22, 0.18) if cuts else 1.0
    array = jax.random.normal(key, shape, jnp.float32) * scale * factor_of
    return jnp.minimum(jnp.maximum(array, -bound), bound).astype(kind)


def setup_inputs(seed: int = 0) -> dict:
    keys = jax.random.split(jax.random.key(seed), 10)
    return {
        "features": scatter_about(keys[0], (NODES, D), 1.0, 6.0, ((0, 32),)),
        "w_one": scatter_about(keys[1], (RELATIONS + 1, D, D), D ** -0.5, 0.25),
        "w_two": scatter_about(keys[2], (RELATIONS, D, CLASSES), D ** -0.5, 0.25),
        "self_two": draw_self_two(jax.random.fold_in(keys[9], 71), 0),
        "edge_src": draw_edge_src(jax.random.fold_in(keys[9], 71), 0),
        "edge_dst": draw_edge_dst(jax.random.fold_in(keys[9], 71), 0),
        "send_rows": set_ends(jax.random.randint(keys[6], (N_DOM, N_DOM, SLOTS), 0, NODES_DEV), jax.random.fold_in(keys[6], 1), 0, NODES_DEV - 1).astype(jnp.int32),
        "send_count": draw_send_count(jax.random.fold_in(keys[9], 71), 0),
        "labels": draw_labels(jax.random.fold_in(keys[9], 71), 0),
    }


loss_scale = 256.0


def slot_rows(values, send_rows, send_count, device):
    picks = send_rows[:, device, :]
    owners = jnp.arange(N_DOM, dtype=jnp.int32)[:, None] * NODES_DEV + picks
    chosen = values[owners.reshape(-1)]
    live_slot = (jnp.arange(SLOTS, dtype=jnp.int32)[None, :] < send_count[:, device][:, None]).reshape(-1)
    return jnp.where(live_slot[:, None], chosen, jnp.zeros_like(chosen))


def device_edges(edge_src, edge_dst, device):
    blocks = NODES_DEV // 128
    start = (device * blocks).astype(jnp.int32)
    return (lax.dynamic_slice_in_dim(edge_src, start, blocks, 1), lax.dynamic_slice_in_dim(edge_dst, start, blocks, 1))


def edge_targets(targets):
    blocks = NODES_DEV // 128
    live_edge = targets >= 0
    node_of = jnp.arange(blocks, dtype=jnp.int32)[None, :, None] * 128 + jnp.where(live_edge, targets, 0)
    segment = jnp.arange(RELATIONS, dtype=jnp.int32)[:, None, None] * NODES_DEV + node_of
    return jnp.where(live_edge, segment, RELATIONS * NODES_DEV).reshape(-1).astype(jnp.int32)


def aggregate(node_table, sources, targets):
    segment = edge_targets(targets)
    slots_all = RELATIONS * NODES_DEV + 1
    gathered = node_table[sources.reshape(-1)].astype(jnp.float32)
    sums = jax.ops.segment_sum(gathered, segment, num_segments=slots_all)[:-1]
    counts = jax.ops.segment_sum(jnp.ones(segment.shape, jnp.float32), segment, num_segments=slots_all)[:-1]
    norm_rows = 1.0 / jnp.maximum(counts, 1.0)
    averaged = (sums * norm_rows[:, None]).astype(jnp.bfloat16)
    return averaged.reshape(RELATIONS, NODES_DEV, -1), norm_rows.reshape(RELATIONS, NODES_DEV)


def layer(device, values, weights, self_weight, send_rows, send_count, edge_src, edge_dst):
    own_rows = lax.dynamic_slice_in_dim(values, (device * NODES_DEV).astype(jnp.int32), NODES_DEV, 0)
    node_table = jnp.concatenate([own_rows, slot_rows(values, send_rows, send_count, device)], axis=0)
    sources, targets = device_edges(edge_src, edge_dst, device)
    averaged, norm_rows = aggregate(node_table, sources, targets)
    output = jnp.einsum('rnd,rde->ne', averaged.astype(jnp.float32), weights.astype(jnp.float32))
    output = output + jnp.dot(own_rows, self_weight, preferred_element_type=jnp.float32)
    return own_rows, averaged, norm_rows, sources, targets, output


def reference(features, w_one, w_two, self_two, edge_src, edge_dst, send_rows, send_count, labels):
    devices = jnp.arange(N_DOM, dtype=jnp.int32)

    def first(device):
        return layer(device, features, w_one[:RELATIONS], w_one[RELATIONS], send_rows, send_count, edge_src, edge_dst)

    def second(device, hidden):
        return layer(device, hidden, w_two, self_two, send_rows, send_count, edge_src, edge_dst)

    hidden = lax.map(lambda device: jnp.maximum(first(device)[5], 0.0).astype(jnp.bfloat16), devices).reshape(NODES, D)
    logits = lax.map(lambda device: second(device, hidden)[5], devices).reshape(NODES, CLASSES)

    labelled = labels >= 0
    log_total = jax.nn.logsumexp(logits, axis=1)
    one_hot = (jnp.arange(CLASSES, dtype=jnp.int32)[None, :] == labels[:, None]).astype(jnp.float32)
    picked = jnp.sum(logits * one_hot, axis=1)
    total = jnp.sum(jnp.where(labelled, log_total - picked, 0.0))
    label_count = jnp.sum(labelled.astype(jnp.float32))
    loss = total / label_count
    softmax_out = jnp.exp(logits - log_total[:, None])
    grad_logits = (loss_scale * (softmax_out - one_hot) * labelled[:, None].astype(jnp.float32) / label_count).astype(jnp.bfloat16)

    table_rows = NODES_DEV + N_DOM * SLOTS

    def back_two(carry, device):
        own_rows, averaged, norm_rows, sources, targets, unused = second(device, hidden)
        grad_rows = lax.dynamic_slice_in_dim(grad_logits, (device * NODES_DEV).astype(jnp.int32), NODES_DEV, 0)
        grad_term = jnp.concatenate([
            jnp.einsum('rnd,nc->rdc', averaged.astype(jnp.float32), grad_rows.astype(jnp.float32)),
            jnp.dot(own_rows.T, grad_rows, preferred_element_type=jnp.float32)[None]], axis=0)
        spread = (jnp.einsum('nc,rdc->rnd', grad_rows.astype(jnp.float32), w_two.astype(jnp.float32)) * norm_rows[:, :, None]).astype(jnp.bfloat16)
        segment = edge_targets(targets)
        padded = jnp.concatenate([spread.reshape(RELATIONS * NODES_DEV, D), jnp.zeros((1, D), jnp.bfloat16)], axis=0)
        per_edge = padded[segment].astype(jnp.float32)
        table_grad = jax.ops.segment_sum(per_edge, sources.reshape(-1), num_segments=table_rows)
        local_grad = table_grad[:NODES_DEV] + jnp.dot(grad_rows, self_two.T, preferred_element_type=jnp.float32)
        return carry + grad_term, (local_grad, table_grad[NODES_DEV:].astype(jnp.bfloat16))

    grad_two, outputs = lax.scan(back_two, jnp.zeros((RELATIONS + 1, D, CLASSES), jnp.float32), devices)
    local_grads, backs = outputs

    owners = jnp.arange(N_DOM, dtype=jnp.int32)[None, :, None] * NODES_DEV + jnp.swapaxes(send_rows, 0, 1)
    live_slot = jnp.arange(SLOTS, dtype=jnp.int32)[None, None, :] < jnp.swapaxes(send_count, 0, 1)[:, :, None]
    back_values = jnp.where(live_slot[..., None], backs.reshape(N_DOM, N_DOM, SLOTS, D).astype(jnp.float32), 0.0)
    returned = jax.ops.segment_sum(back_values.reshape(-1, D), owners.reshape(-1), num_segments=NODES)
    grad_hidden = local_grads.reshape(NODES, D) + returned

    def back_one(carry, device):
        own_rows, averaged, norm_rows, sources, targets, before_relu = first(device)
        grad_rows = lax.dynamic_slice_in_dim(grad_hidden, (device * NODES_DEV).astype(jnp.int32), NODES_DEV, 0)
        grad_pre = jnp.where(before_relu > 0.0, grad_rows, 0.0).astype(jnp.bfloat16)
        grad_term = jnp.concatenate([
            jnp.einsum('rnd,ne->rde', averaged.astype(jnp.float32), grad_pre.astype(jnp.float32)),
            jnp.dot(own_rows.T, grad_pre, preferred_element_type=jnp.float32)[None]], axis=0)
        return carry + grad_term, None

    grad_one, unused = lax.scan(back_one, jnp.zeros((RELATIONS + 1, D, D), jnp.float32), devices)
    return (logits, loss, grad_one.reshape((RELATIONS + 1) * D, D), grad_two.reshape((RELATIONS + 1) * D, CLASSES))
```

```python
import jax
import jax.numpy as jnp
from jax import lax
from jax.sharding import PartitionSpec as P

loss_scale = 256.0
f32 = jnp.float32
bf16 = jnp.bfloat16


def exchange(rows, peers, slots):
    sent = rows.reshape(peers, slots, -1)
    got = lax.all_to_all(sent, "dom", split_axis=0, concat_axis=0, tiled=True)
    return got.reshape(peers * slots, -1)


def all_sum(value):
    spread = jnp.broadcast_to(value, (1, 128))
    return jnp.sum(lax.all_gather(spread, "dom", axis=0, tiled=True)[:, 0])


def on_device(features, w_one, w_two, self_two, edge_src, edge_dst, send_rows, send_count, labels):
    peers = lax.axis_size("dom")
    node_rows, width = features.shape
    relations, blocks, edges = edge_src.shape
    slots = send_rows.shape[2]
    table_rows = node_rows + peers * slots
    labelled = labels >= 0
    label_count = all_sum(jnp.sum(labelled.astype(f32)))

    live = jnp.arange(slots, dtype=jnp.int32)[None, :] < send_count[0][:, None]
    picks = jnp.where(live, send_rows[0], -1).reshape(-1)
    select = (picks[:, None] == jnp.arange(node_rows, dtype=jnp.int32)[None, :]).astype(bf16)

    arrived = exchange(jnp.dot(select, features), peers, slots)
    hot_dst = edge_dst[:, :, None, :] == jnp.arange(128, dtype=jnp.int32)[None, None, :, None]
    hot_src = edge_src[:, :, None, :] == jnp.arange(table_rows, dtype=jnp.int32)[None, None, :, None]
    counts = jnp.einsum(
        "rbve,rbte->rbvt", hot_dst.astype(bf16), hot_src.astype(bf16), preferred_element_type=f32
    )
    adj = counts.astype(bf16).reshape(relations * blocks * 128, table_rows)
    norm = 1.0 / jnp.maximum(jnp.sum(hot_dst.astype(f32), axis=3), 1.0)
    norm = norm.reshape(relations * blocks * 128, 1)

    def averages(own, got):
        table = jnp.concatenate([own, got], axis=0)
        sums = jnp.dot(adj, table, preferred_element_type=f32)
        return (sums * norm).astype(bf16).reshape(relations, node_rows, width)

    avg_one = jnp.concatenate([averages(features, arrived), features[None]], axis=0)
    pre = jnp.einsum("rnd,rde->ne", avg_one, w_one, preferred_element_type=f32)
    hidden = jnp.maximum(pre, 0.0).astype(bf16)
    arrived_hidden = exchange(jnp.dot(select, hidden), peers, slots)
    avg_two = jnp.concatenate([averages(hidden, arrived_hidden), hidden[None]], axis=0)
    w_all = jnp.concatenate([w_two, self_two[None]], axis=0)
    logits = jnp.einsum("rnd,rdc->nc", avg_two, w_all, preferred_element_type=f32)

    classes = logits.shape[1]
    log_total = jax.nn.logsumexp(logits, axis=1)
    one_hot = (jnp.arange(classes, dtype=jnp.int32)[None, :] == labels[:, None]).astype(f32)
    picked = jnp.sum(logits * one_hot, axis=1)
    local_total = jnp.sum(jnp.where(labelled, log_total - picked, 0.0))
    softmax_out = jnp.exp(logits - log_total[:, None])
    grad_logits = (
        loss_scale * (softmax_out - one_hot) * labelled[:, None].astype(f32) / label_count
    ).astype(bf16)

    def scattered(left, right):
        full = jnp.einsum("rnd,nc->rdc", left, right, preferred_element_type=f32)
        full = full.astype(bf16).reshape((relations + 1) * width, -1)
        return lax.psum_scatter(full, "dom", scatter_dimension=0, tiled=True).astype(f32)

    grad_two = scattered(avg_two, grad_logits)
    spread = jnp.einsum("nc,rdc->rnd", grad_logits, w_two, preferred_element_type=f32)
    spread = (spread.reshape(-1, width) * norm).astype(bf16)
    table_grad = lax.dot_general(adj, spread, (((0,), (0,)), ((), ())), preferred_element_type=f32)
    local_grad = table_grad[:node_rows] + jnp.dot(
        grad_logits, self_two.T, preferred_element_type=f32
    )
    returned = exchange(table_grad[node_rows:].astype(bf16), peers, slots)
    grad_hidden = local_grad + lax.dot_general(
        select, returned, (((0,), (0,)), ((), ())), preferred_element_type=f32
    )
    grad_pre = jnp.where(pre > 0.0, grad_hidden, 0.0).astype(bf16)
    grad_one = scattered(avg_one, grad_pre)
    loss = all_sum(local_total) / label_count
    return (logits, loss, grad_one, grad_two)


def solution(mesh):
    in_specs = (
        P("dom", None),
        P(),
        P(),
        P(),
        P(None, "dom", None),
        P(None, "dom", None),
        P("dom", None, None),
        P("dom", None),
        P("dom"),
    )
    out_specs = (P("dom", None), P(), P("dom", None), P("dom", None))
    return jax.shard_map(
        on_device, mesh=mesh, in_specs=in_specs, out_specs=out_specs, check_vma=False
    )
```

```python
import functools

import jax
import jax.numpy as jnp
from jax import lax
from jax.experimental import pallas as pl
from jax.experimental.pallas import tpu as pltpu
from jax.sharding import PartitionSpec as P

loss_scale = 256.0
f32 = jnp.float32
bf16 = jnp.bfloat16
MESH = pl.DeviceIdType.MESH


def exchange_kernel(peers, rows_ref, stat_ref, got_ref, stats_ref, send_sem, recv_sem, stat_send, stat_recv, own_sem):
    me = lax.axis_index("dom")
    barrier = pltpu.get_barrier_semaphore()
    for step in range(1, peers):
        peer = lax.rem(me + step, peers)
        pl.semaphore_signal(barrier, inc=1, device_id=(peer,), device_id_type=MESH)
    own = pltpu.make_async_copy(rows_ref.at[me], got_ref.at[me], own_sem)
    own.start()
    stats_ref[me] = stat_ref[...]
    pl.semaphore_wait(barrier, peers - 1)
    copies = []
    for step in range(1, peers):
        peer = lax.rem(me + step, peers)
        copies.append(
            pltpu.make_async_remote_copy(
                src_ref=rows_ref.at[peer],
                dst_ref=got_ref.at[me],
                send_sem=send_sem.at[step],
                recv_sem=recv_sem.at[step],
                device_id=(peer,),
                device_id_type=MESH,
            )
        )
        copies.append(
            pltpu.make_async_remote_copy(
                src_ref=stat_ref,
                dst_ref=stats_ref.at[me],
                send_sem=stat_send.at[step],
                recv_sem=stat_recv.at[step],
                device_id=(peer,),
                device_id_type=MESH,
            )
        )
        copies[-2].start()
        copies[-1].start()
    for copy in copies:
        copy.wait_recv()
    for copy in copies:
        copy.wait_send()
    own.wait()


def exchange(rows, stat, peers, slots, call):
    width = rows.shape[1]
    stat = jnp.broadcast_to(stat.astype(f32), (8, 128))
    got, stats = pl.pallas_call(
        functools.partial(exchange_kernel, peers),
        out_shape=[
            jax.ShapeDtypeStruct((peers, slots, width), bf16),
            jax.ShapeDtypeStruct((peers, 8, 128), f32),
        ],
        in_specs=[pl.BlockSpec(memory_space=pltpu.VMEM)] * 2,
        out_specs=[pl.BlockSpec(memory_space=pltpu.VMEM)] * 2,
        scratch_shapes=[pltpu.SemaphoreType.DMA((peers,))] * 4 + [pltpu.SemaphoreType.DMA],
        compiler_params=pltpu.CompilerParams(
            collective_id=call, has_side_effects=True, vmem_limit_bytes=8 * 1024 * 1024
        ),
        name=f"exchange_{call}",
    )(rows.reshape(peers, slots, width), stat)
    return got.reshape(peers * slots, width), jnp.sum(stats[:, 0, 0])


def bit_orders(bits):
    links = list(range(1, bits))
    swapped = links[1::-1] + links[2:]
    return links, swapped


def placed(chunk, order):
    spot = 0
    for bit in order:
        spot = spot * 2 + ((chunk >> (bit - 1)) & 1)
    return spot


def scatter_kernel(stripes, bits, *refs):
    count = len(stripes)
    parts, outs, rest = refs[:2], refs[2:4], refs[4:]
    sums, gots, send_sem, recv_sem = rest[:bits - 1], rest[bits - 1:2 * bits - 1], rest[-2], rest[-1]
    me = lax.axis_index("dom")
    barrier = pltpu.get_barrier_semaphore()

    def side(bit):
        return lax.rem(me // (1 << bit), 2)

    def partner(bit):
        return me + (1 << bit) * (1 - 2 * side(bit))

    for bit in range(bits):
        pl.semaphore_signal(barrier, inc=1, device_id=(partner(bit),), device_id_type=MESH)
    pl.semaphore_wait(barrier, bits)

    def copy_of(stripe, level):
        which, lane, order = stripes[stripe]
        if level == 0:
            bit = 0
            source = parts[which].at[:, 1 - side(0), :, pl.ds(lane, 128)]
        else:
            bit = order[level - 1]
            half = 1 << (bits - 1 - level)
            source = sums[level - 1].at[stripe, pl.ds((1 - side(bit)) * half, half)]
        return pltpu.make_async_remote_copy(
            src_ref=source,
            dst_ref=gots[level].at[stripe],
            send_sem=send_sem.at[stripe, level],
            recv_sem=recv_sem.at[stripe, level],
            device_id=(partner(bit),),
            device_id_type=MESH,
        )

    def add_up(stripe, level):
        which, lane, order = stripes[stripe]
        if level == 0:
            for chunk in range(1 << (bits - 1)):
                own = parts[which][chunk, side(0), :, pl.ds(lane, 128)].astype(f32)
                total = own + gots[0][stripe, chunk].astype(f32)
                sums[0][stripe, placed(chunk, order)] = total.astype(bf16)
            return
        bit = order[level - 1]
        half = 1 << (bits - 1 - level)
        own = sums[level - 1][stripe, pl.ds(side(bit) * half, half)].astype(f32)
        total = own + gots[level][stripe].astype(f32)
        if level < bits - 1:
            sums[level][stripe] = total.astype(bf16)
        else:
            outs[which][:, pl.ds(lane, 128)] = total[0]

    for stripe in range(count):
        copy_of(stripe, 0).start()
    for level in range(bits):
        for stripe in range(count):
            copy_of(stripe, level).wait_recv()
            add_up(stripe, level)
            if level < bits - 1:
                copy_of(stripe, level + 1).start()
    for level in range(bits):
        for stripe in range(count):
            copy_of(stripe, level).wait_send()


def scatter_sums(first, second, peers):
    bits = peers.bit_length() - 1
    rows = first.shape[0] // peers
    orders = bit_orders(bits)
    stripes = []
    for which, part in enumerate((first, second)):
        for lane in range(0, part.shape[1], 128):
            stripes.append((which, lane, orders[len(stripes) % 2]))
    count = len(stripes)
    half = peers // 2
    sums = [pltpu.VMEM((count, half >> k, rows, 128), bf16) for k in range(bits - 1)]
    gots = [pltpu.VMEM((count, half >> k, rows, 128), bf16) for k in range(bits)]
    views = [part.reshape(half, 2, rows, part.shape[1]) for part in (first, second)]
    return pl.pallas_call(
        functools.partial(scatter_kernel, stripes, bits),
        out_shape=[jax.ShapeDtypeStruct((rows, part.shape[1]), f32) for part in (first, second)],
        in_specs=[pl.BlockSpec(memory_space=pltpu.VMEM)] * 2,
        out_specs=[pl.BlockSpec(memory_space=pltpu.VMEM)] * 2,
        scratch_shapes=sums + gots + [
            pltpu.SemaphoreType.DMA((count, bits)),
            pltpu.SemaphoreType.DMA((count, bits)),
        ],
        compiler_params=pltpu.CompilerParams(
            collective_id=0, has_side_effects=True, vmem_limit_bytes=60 * 1024 * 1024
        ),
        name="scatter_sums",
    )(*views)


def on_device(features, w_one, w_two, self_two, edge_src, edge_dst, send_rows, send_count, labels):
    peers = lax.axis_size("dom")
    node_rows, width = features.shape
    relations, blocks, edges = edge_src.shape
    slots = send_rows.shape[2]
    table_rows = node_rows + peers * slots
    labelled = labels >= 0
    local_count = jnp.sum(labelled.astype(f32))

    live = jnp.arange(slots, dtype=jnp.int32)[None, :] < send_count[0][:, None]
    picks = jnp.where(live, send_rows[0], -1).reshape(-1)
    select = (picks[:, None] == jnp.arange(node_rows, dtype=jnp.int32)[None, :]).astype(bf16)

    arrived, label_count = exchange(jnp.dot(select, features), local_count, peers, slots, 1)
    hot_dst = edge_dst[:, :, None, :] == jnp.arange(128, dtype=jnp.int32)[None, None, :, None]
    hot_src = edge_src[:, :, None, :] == jnp.arange(table_rows, dtype=jnp.int32)[None, None, :, None]
    counts = jnp.einsum(
        "rbve,rbte->rbvt", hot_dst.astype(bf16), hot_src.astype(bf16), preferred_element_type=f32
    )
    adj = counts.astype(bf16).reshape(relations * blocks * 128, table_rows)
    norm = 1.0 / jnp.maximum(jnp.sum(hot_dst.astype(f32), axis=3), 1.0)
    norm = norm.reshape(relations * blocks * 128, 1)

    def averages(own, got):
        table = jnp.concatenate([own, got], axis=0)
        sums = jnp.dot(adj, table, preferred_element_type=f32)
        return (sums * norm).astype(bf16).reshape(relations, node_rows, width)

    avg_one = jnp.concatenate([averages(features, arrived), features[None]], axis=0)
    pre = jnp.einsum("rnd,rde->ne", avg_one, w_one, preferred_element_type=f32)
    hidden = jnp.maximum(pre, 0.0).astype(bf16)
    arrived_hidden, unused = exchange(jnp.dot(select, hidden), local_count, peers, slots, 2)
    avg_two = jnp.concatenate([averages(hidden, arrived_hidden), hidden[None]], axis=0)
    w_all = jnp.concatenate([w_two, self_two[None]], axis=0)
    logits = jnp.einsum("rnd,rdc->nc", avg_two, w_all, preferred_element_type=f32)

    classes = logits.shape[1]
    log_total = jax.nn.logsumexp(logits, axis=1)
    one_hot = (jnp.arange(classes, dtype=jnp.int32)[None, :] == labels[:, None]).astype(f32)
    picked = jnp.sum(logits * one_hot, axis=1)
    local_total = jnp.sum(jnp.where(labelled, log_total - picked, 0.0))
    softmax_out = jnp.exp(logits - log_total[:, None])
    grad_logits = (
        loss_scale * (softmax_out - one_hot) * labelled[:, None].astype(f32) / label_count
    ).astype(bf16)

    def products(left, right):
        full = jnp.einsum("rnd,nc->rdc", left, right, preferred_element_type=f32)
        return full.astype(bf16).reshape((relations + 1) * width, -1)

    padded = jnp.pad(grad_logits, ((0, 0), (0, -classes % 128)))
    part_two = products(avg_two, padded)
    spread = jnp.einsum("nc,rdc->rnd", grad_logits, w_two, preferred_element_type=f32)
    spread = (spread.reshape(-1, width) * norm).astype(bf16)
    table_grad = lax.dot_general(adj, spread, (((0,), (0,)), ((), ())), preferred_element_type=f32)
    local_grad = table_grad[:node_rows] + jnp.dot(
        grad_logits, self_two.T, preferred_element_type=f32
    )
    returned, total = exchange(table_grad[node_rows:].astype(bf16), local_total, peers, slots, 3)
    grad_hidden = local_grad + lax.dot_general(
        select, returned, (((0,), (0,)), ((), ())), preferred_element_type=f32
    )
    grad_pre = jnp.where(pre > 0.0, grad_hidden, 0.0).astype(bf16)
    grad_one, grad_two = scatter_sums(products(avg_one, grad_pre), part_two, peers)
    return (logits, total / label_count, grad_one, grad_two[:, :classes])


def solution(mesh):
    in_specs = (
        P("dom", None),
        P(),
        P(),
        P(),
        P(None, "dom", None),
        P(None, "dom", None),
        P("dom", None, None),
        P("dom", None),
        P("dom"),
    )
    out_specs = (P("dom", None), P(), P("dom", None), P("dom", None))
    return jax.shard_map(
        on_device, mesh=mesh, in_specs=in_specs, out_specs=out_specs, check_vma=False
    )
```

```python
import functools

import jax
import jax.numpy as jnp
from jax import lax
from jax.experimental import pallas as pl
from jax.experimental.pallas import tpu as pltpu
from jax.sharding import PartitionSpec as P

loss_scale = 256.0
f32 = jnp.float32
bf16 = jnp.bfloat16
MESH = pl.DeviceIdType.MESH


def exchange_kernel(peers, rows_ref, stat_ref, got_ref, stats_ref, send_sem, recv_sem, stat_send, stat_recv, own_sem):
    me = lax.axis_index("dom")
    barrier = pltpu.get_barrier_semaphore()
    for step in range(1, peers):
        peer = lax.rem(me + step, peers)
        pl.semaphore_signal(barrier, inc=1, device_id=(peer,), device_id_type=MESH)
    own = pltpu.make_async_copy(rows_ref.at[me], got_ref.at[me], own_sem)
    own.start()
    stats_ref[me] = stat_ref[...]
    pl.semaphore_wait(barrier, peers - 1)
    copies = []
    for step in range(1, peers):
        peer = lax.rem(me + step, peers)
        copies.append(
            pltpu.make_async_remote_copy(
                src_ref=rows_ref.at[peer],
                dst_ref=got_ref.at[me],
                send_sem=send_sem.at[step],
                recv_sem=recv_sem.at[step],
                device_id=(peer,),
                device_id_type=MESH,
            )
        )
        copies.append(
            pltpu.make_async_remote_copy(
                src_ref=stat_ref,
                dst_ref=stats_ref.at[me],
                send_sem=stat_send.at[step],
                recv_sem=stat_recv.at[step],
                device_id=(peer,),
                device_id_type=MESH,
            )
        )
        copies[-2].start()
        copies[-1].start()
    for copy in copies:
        copy.wait_recv()
    for copy in copies:
        copy.wait_send()
    own.wait()


def exchange(rows, stat, peers, slots, call):
    width = rows.shape[1]
    stat = jnp.broadcast_to(stat.astype(f32), (1, 128))
    got, stats = pl.pallas_call(
        functools.partial(exchange_kernel, peers),
        out_shape=[
            jax.ShapeDtypeStruct((peers, slots, width), bf16),
            jax.ShapeDtypeStruct((peers, 1, 128), f32),
        ],
        in_specs=[pl.BlockSpec(memory_space=pltpu.VMEM)] * 2,
        out_specs=[pl.BlockSpec(memory_space=pltpu.VMEM)] * 2,
        scratch_shapes=[pltpu.SemaphoreType.DMA((peers,))] * 4 + [pltpu.SemaphoreType.DMA],
        compiler_params=pltpu.CompilerParams(
            collective_id=call, has_side_effects=True, vmem_limit_bytes=8 * 1024 * 1024
        ),
        name=f"exchange_{call}",
    )(rows.reshape(peers, slots, width), stat)
    return got.reshape(peers * slots, width), jnp.sum(stats[:, 0, 0])


def bit_orders(bits):
    links = list(range(1, bits))
    swapped = links[1::-1] + links[2:]
    return links, swapped, links[2:] + links[:2]


def placed(chunk, order):
    spot = 0
    for bit in order:
        spot = spot * 2 + ((chunk >> (bit - 1)) & 1)
    return spot


def scatter_kernel(stripes, bits, *refs):
    count = len(stripes)
    parts, outs, rest = refs[:2], refs[2:4], refs[4:]
    sums, gots, send_sem, recv_sem = rest[:bits - 1], rest[bits - 1:2 * bits - 1], rest[-2], rest[-1]
    me = lax.axis_index("dom")
    barrier = pltpu.get_barrier_semaphore()

    def side(bit):
        return lax.rem(me // (1 << bit), 2)

    def partner(bit):
        return me + (1 << bit) * (1 - 2 * side(bit))

    for bit in range(bits):
        pl.semaphore_signal(barrier, inc=1, device_id=(partner(bit),), device_id_type=MESH)
    pl.semaphore_wait(barrier, bits)

    def copy_of(stripe, level):
        which, lane, order = stripes[stripe]
        if level == 0:
            bit = 0
            source = parts[which].at[:, 1 - side(0), :, pl.ds(lane, 128)]
        else:
            bit = order[level - 1]
            half = 1 << (bits - 1 - level)
            source = sums[level - 1].at[stripe, pl.ds((1 - side(bit)) * half, half)]
        return pltpu.make_async_remote_copy(
            src_ref=source,
            dst_ref=gots[level].at[stripe],
            send_sem=send_sem.at[stripe, level],
            recv_sem=recv_sem.at[stripe, level],
            device_id=(partner(bit),),
            device_id_type=MESH,
        )

    def add_up(stripe, level):
        which, lane, order = stripes[stripe]
        if level == 0:
            for chunk in range(1 << (bits - 1)):
                own = parts[which][chunk, side(0), :, pl.ds(lane, 128)].astype(f32)
                total = own + gots[0][stripe, chunk].astype(f32)
                sums[0][stripe, placed(chunk, order)] = total.astype(bf16)
            return
        bit = order[level - 1]
        half = 1 << (bits - 1 - level)
        own = sums[level - 1][stripe, pl.ds(side(bit) * half, half)].astype(f32)
        total = own + gots[level][stripe].astype(f32)
        if level < bits - 1:
            sums[level][stripe] = total.astype(bf16)
        else:
            outs[which][:, pl.ds(lane, 128)] = total[0]

    for stripe in range(count):
        copy_of(stripe, 0).start()
    units = [list(range(0, 3))] + [list(range(k, min(k + 2, count))) for k in range(3, count, 2)]
    for wave in range(len(units) + bits - 1):
        for level in range(bits):
            for stripe in units[wave - level] if 0 <= wave - level < len(units) else ():
                copy_of(stripe, level).wait_recv()
                add_up(stripe, level)
                if level < bits - 1:
                    copy_of(stripe, level + 1).start()
    for level in range(bits):
        for stripe in range(count):
            copy_of(stripe, level).wait_send()


def scatter_sums(first, second, peers):
    bits = peers.bit_length() - 1
    rows = first.shape[0] // peers
    orders = bit_orders(bits)
    stripes = []
    for which, part in enumerate((first, second)):
        for lane in range(0, part.shape[1], 128):
            stripes.append((which, lane, orders[len(stripes) % 2 if stripes else 2]))
    count = len(stripes)
    half = peers // 2
    sums = [pltpu.VMEM((count, half >> k, rows, 128), bf16) for k in range(bits - 1)]
    gots = [pltpu.VMEM((count, half >> k, rows, 128), bf16) for k in range(bits)]
    views = [part.reshape(half, 2, rows, part.shape[1]) for part in (first, second)]
    return pl.pallas_call(
        functools.partial(scatter_kernel, stripes, bits),
        out_shape=[jax.ShapeDtypeStruct((rows, part.shape[1]), f32) for part in (first, second)],
        in_specs=[pl.BlockSpec(memory_space=pltpu.VMEM)] * 2,
        out_specs=[pl.BlockSpec(memory_space=pltpu.VMEM)] * 2,
        scratch_shapes=sums + gots + [
            pltpu.SemaphoreType.DMA((count, bits)),
            pltpu.SemaphoreType.DMA((count, bits)),
        ],
        compiler_params=pltpu.CompilerParams(
            collective_id=0, has_side_effects=True, vmem_limit_bytes=60 * 1024 * 1024
        ),
        name="scatter_sums",
    )(*views)


def on_device(features, w_one, w_two, self_two, edge_src, edge_dst, send_rows, send_count, labels):
    peers = lax.axis_size("dom")
    node_rows, width = features.shape
    relations, blocks, edges = edge_src.shape
    slots = send_rows.shape[2]
    table_rows = node_rows + peers * slots
    labelled = labels >= 0
    local_count = jnp.sum(labelled.astype(f32))

    live = jnp.arange(slots, dtype=jnp.int32)[None, :] < send_count[0][:, None]
    picks = jnp.where(live, send_rows[0], -1).reshape(-1)
    select = (picks[:, None] == jnp.arange(node_rows, dtype=jnp.int32)[None, :]).astype(bf16)

    arrived, label_count = exchange(jnp.dot(select, features), local_count, peers, slots, 1)
    hot_dst = edge_dst[:, :, None, :] == jnp.arange(128, dtype=jnp.int32)[None, None, :, None]
    hot_src = edge_src[:, :, None, :] == jnp.arange(table_rows, dtype=jnp.int32)[None, None, :, None]
    counts = jnp.einsum(
        "rbve,rbte->rbvt", hot_dst.astype(bf16), hot_src.astype(bf16), preferred_element_type=f32
    )
    adj = counts.astype(bf16).reshape(relations * blocks * 128, table_rows)
    norm = 1.0 / jnp.maximum(jnp.sum(hot_dst.astype(f32), axis=3), 1.0)
    norm = norm.reshape(relations * blocks * 128, 1)

    def averages(own, got):
        table = jnp.concatenate([own, got], axis=0)
        sums = jnp.dot(adj, table, preferred_element_type=f32)
        return (sums * norm).astype(bf16).reshape(relations, node_rows, width)

    avg_one = jnp.concatenate([averages(features, arrived), features[None]], axis=0)
    pre = jnp.einsum("rnd,rde->ne", avg_one, w_one, preferred_element_type=f32)
    hidden = jnp.maximum(pre, 0.0).astype(bf16)
    arrived_hidden, unused = exchange(jnp.dot(select, hidden), local_count, peers, slots, 2)
    avg_two = jnp.concatenate([averages(hidden, arrived_hidden), hidden[None]], axis=0)
    w_all = jnp.concatenate([w_two, self_two[None]], axis=0)
    logits = jnp.einsum("rnd,rdc->nc", avg_two, w_all, preferred_element_type=f32)

    classes = logits.shape[1]
    log_total = jax.nn.logsumexp(logits, axis=1)
    one_hot = (jnp.arange(classes, dtype=jnp.int32)[None, :] == labels[:, None]).astype(f32)
    picked = jnp.sum(logits * one_hot, axis=1)
    local_total = jnp.sum(jnp.where(labelled, log_total - picked, 0.0))
    softmax_out = jnp.exp(logits - log_total[:, None])
    grad_logits = (
        loss_scale * (softmax_out - one_hot) * labelled[:, None].astype(f32) / label_count
    ).astype(bf16)

    def products(left, right):
        full = jnp.einsum("rnd,nc->rdc", left, right, preferred_element_type=f32)
        return full.astype(bf16).reshape((relations + 1) * width, -1)

    padded = jnp.pad(grad_logits, ((0, 0), (0, -classes % 128)))
    part_two = products(avg_two, padded)
    spread = jnp.einsum("nc,rdc->rnd", grad_logits, w_two, preferred_element_type=f32)
    spread = (spread.reshape(-1, width) * norm).astype(bf16)
    table_grad = lax.dot_general(adj, spread, (((0,), (0,)), ((), ())), preferred_element_type=f32)
    local_grad = table_grad[:node_rows] + jnp.dot(
        grad_logits, self_two.T, preferred_element_type=f32
    )
    returned, total = exchange(table_grad[node_rows:].astype(bf16), local_total, peers, slots, 3)
    grad_hidden = local_grad + lax.dot_general(
        select, returned, (((0,), (0,)), ((), ())), preferred_element_type=f32
    )
    grad_pre = jnp.where(pre > 0.0, grad_hidden, 0.0).astype(bf16)
    grad_one, grad_two = scatter_sums(products(avg_one, grad_pre), part_two, peers)
    return (logits, total / label_count, grad_one, grad_two[:, :classes])


def solution(mesh):
    in_specs = (
        P("dom", None),
        P(),
        P(),
        P(),
        P(None, "dom", None),
        P(None, "dom", None),
        P("dom", None, None),
        P("dom", None),
        P("dom"),
    )
    out_specs = (P("dom", None), P(), P("dom", None), P("dom", None))
    return jax.shard_map(
        on_device, mesh=mesh, in_specs=in_specs, out_specs=out_specs, check_vma=False
    )
```

```python
import functools

import jax
import jax.numpy as jnp
from jax import lax
from jax.experimental import pallas as pl
from jax.experimental.pallas import tpu as pltpu
from jax.sharding import PartitionSpec as P

loss_scale = 256.0
f32 = jnp.float32
bf16 = jnp.bfloat16
MESH = pl.DeviceIdType.MESH


def exchange_kernel(peers, rows_ref, stat_ref, got_ref, stats_ref, send_sem, recv_sem, stat_send, stat_recv, own_sem):
    me = lax.axis_index("dom")
    barrier = pltpu.get_barrier_semaphore()
    for step in range(1, peers):
        peer = lax.rem(me + step, peers)
        pl.semaphore_signal(barrier, inc=1, device_id=(peer,), device_id_type=MESH)
    own = pltpu.make_async_copy(rows_ref.at[me], got_ref.at[me], own_sem)
    own.start()
    stats_ref[me] = stat_ref[...]
    pl.semaphore_wait(barrier, peers - 1)
    copies = []
    for step in range(1, peers):
        peer = lax.rem(me + step, peers)
        copies.append(
            pltpu.make_async_remote_copy(
                src_ref=rows_ref.at[peer],
                dst_ref=got_ref.at[me],
                send_sem=send_sem.at[step],
                recv_sem=recv_sem.at[step],
                device_id=(peer,),
                device_id_type=MESH,
            )
        )
        copies.append(
            pltpu.make_async_remote_copy(
                src_ref=stat_ref,
                dst_ref=stats_ref.at[me],
                send_sem=stat_send.at[step],
                recv_sem=stat_recv.at[step],
                device_id=(peer,),
                device_id_type=MESH,
            )
        )
        copies[-2].start()
        copies[-1].start()
    for copy in copies:
        copy.wait_recv()
    for copy in copies:
        copy.wait_send()
    own.wait()


def exchange(rows, stat, peers, slots, call):
    width = rows.shape[1]
    stat = jnp.broadcast_to(stat.astype(f32), (1, 128))
    got, stats = pl.pallas_call(
        functools.partial(exchange_kernel, peers),
        out_shape=[
            jax.ShapeDtypeStruct((peers, slots, width), bf16),
            jax.ShapeDtypeStruct((peers, 1, 128), f32),
        ],
        in_specs=[pl.BlockSpec(memory_space=pltpu.VMEM)] * 2,
        out_specs=[pl.BlockSpec(memory_space=pltpu.VMEM)] * 2,
        scratch_shapes=[pltpu.SemaphoreType.DMA((peers,))] * 4 + [pltpu.SemaphoreType.DMA],
        compiler_params=pltpu.CompilerParams(
            collective_id=call, has_side_effects=True, vmem_limit_bytes=8 * 1024 * 1024
        ),
        name=f"exchange_{call}",
    )(rows.reshape(peers, slots, width), stat)
    return got.reshape(peers * slots, width), jnp.sum(stats[:, 0, 0])


def bit_orders(bits):
    links = list(range(1, bits))
    swapped = links[1::-1] + links[2:]
    return links, swapped, links[2:] + links[:2]


def placed(chunk, order):
    spot = 0
    for bit in order:
        spot = spot * 2 + ((chunk >> (bit - 1)) & 1)
    return spot


def scatter_kernel(stripes, bits, *refs):
    count = len(stripes)
    parts, outs, rest = refs[:2], refs[2:4], refs[4:]
    sums, gots, send_sem, recv_sem = rest[:bits - 1], rest[bits - 1:2 * bits - 1], rest[-2], rest[-1]
    me = lax.axis_index("dom")
    barrier = pltpu.get_barrier_semaphore()

    def side(bit):
        return lax.rem(me // (1 << bit), 2)

    def partner(bit):
        return me + (1 << bit) * (1 - 2 * side(bit))

    for bit in range(bits):
        pl.semaphore_signal(barrier, inc=1, device_id=(partner(bit),), device_id_type=MESH)
    pl.semaphore_wait(barrier, bits)

    def copy_of(stripe, level):
        which, lane, order = stripes[stripe]
        if level == 0:
            bit = 0
            source = parts[which].at[:, 1 - side(0), :, pl.ds(lane, 128)]
        else:
            bit = order[level - 1]
            half = 1 << (bits - 1 - level)
            source = sums[level - 1].at[stripe, pl.ds((1 - side(bit)) * half, half)]
        return pltpu.make_async_remote_copy(
            src_ref=source,
            dst_ref=gots[level].at[stripe],
            send_sem=send_sem.at[stripe, level],
            recv_sem=recv_sem.at[stripe, level],
            device_id=(partner(bit),),
            device_id_type=MESH,
        )

    def add_up(stripe, level):
        which, lane, order = stripes[stripe]
        if level == 0:
            for chunk in range(1 << (bits - 1)):
                own = parts[which][chunk, side(0), :, pl.ds(lane, 128)].astype(f32)
                total = own + gots[0][stripe, chunk].astype(f32)
                sums[0][stripe, placed(chunk, order)] = total.astype(bf16)
            return
        bit = order[level - 1]
        half = 1 << (bits - 1 - level)
        own = sums[level - 1][stripe, pl.ds(side(bit) * half, half)].astype(f32)
        total = own + gots[level][stripe].astype(f32)
        if level < bits - 1:
            sums[level][stripe] = total.astype(bf16)
        else:
            outs[which][:, pl.ds(lane, 128)] = total[0]

    for stripe in range(count):
        copy_of(stripe, 0).start()
    units = [list(range(0, 3))] + [list(range(k, min(k + 2, count))) for k in range(3, count, 2)]
    for wave in range(len(units) + bits - 1):
        for level in range(bits):
            for stripe in units[wave - level] if 0 <= wave - level < len(units) else ():
                copy_of(stripe, level).wait_recv()
                add_up(stripe, level)
                if level < bits - 1:
                    copy_of(stripe, level + 1).start()
    for level in range(bits):
        for stripe in range(count):
            copy_of(stripe, level).wait_send()


def scatter_sums(first, second, peers):
    bits = peers.bit_length() - 1
    rows = first.shape[0] // peers
    orders = bit_orders(bits)
    stripes = []
    for which, part in enumerate((first, second)):
        for lane in range(0, part.shape[1], 128):
            stripes.append((which, lane, orders[len(stripes) % 2 if stripes else 2]))
    count = len(stripes)
    half = peers // 2
    sums = [pltpu.VMEM((count, half >> k, rows, 128), bf16) for k in range(bits - 1)]
    gots = [pltpu.VMEM((count, half >> k, rows, 128), bf16) for k in range(bits)]
    views = [part.reshape(half, 2, rows, part.shape[1]) for part in (first, second)]
    return pl.pallas_call(
        functools.partial(scatter_kernel, stripes, bits),
        out_shape=[jax.ShapeDtypeStruct((rows, part.shape[1]), f32) for part in (first, second)],
        in_specs=[pl.BlockSpec(memory_space=pltpu.VMEM)] * 2,
        out_specs=[pl.BlockSpec(memory_space=pltpu.VMEM)] * 2,
        scratch_shapes=sums + gots + [
            pltpu.SemaphoreType.DMA((count, bits)),
            pltpu.SemaphoreType.DMA((count, bits)),
        ],
        compiler_params=pltpu.CompilerParams(
            collective_id=0, has_side_effects=True, vmem_limit_bytes=60 * 1024 * 1024
        ),
        name="scatter_sums",
    )(*views)


def tail_kernel(
    stripes, bits, relations,
    two_ref, back_ref, stat_ref, local_ref, pre_ref, select_ref, avg_ref,
    one_out, two_out, stats_ref, one_ref, grad_ref, got_ref, *rest
):
    peers = 1 << bits
    sums, gots = rest[:bits - 1], rest[bits - 1:2 * bits - 1]
    send_sem, recv_sem, row_send, row_recv, stat_send, stat_recv, own_sem = rest[2 * bits - 1:]
    parts, outs = (two_ref, one_ref), (two_out, one_out)
    rows, width = one_ref.shape[2:]
    me = lax.axis_index("dom")
    barrier = pltpu.get_barrier_semaphore()
    for step in range(1, peers):
        peer = lax.rem(me + step, peers)
        pl.semaphore_signal(barrier, inc=1, device_id=(peer,), device_id_type=MESH)
    own = pltpu.make_async_copy(back_ref.at[me], got_ref.at[me], own_sem)
    own.start()
    stats_ref[me] = stat_ref[...]
    pl.semaphore_wait(barrier, peers - 1)

    def side(bit):
        return lax.rem(me // (1 << bit), 2)

    def copy_of(stripe, level):
        which, lane, order = stripes[stripe]
        if level == 0:
            bit = 0
            source = parts[which].at[:, 1 - side(0), :, pl.ds(lane, 128)]
        else:
            bit = order[level - 1]
            half = 1 << (bits - 1 - level)
            source = sums[level - 1].at[stripe, pl.ds((1 - side(bit)) * half, half)]
        return pltpu.make_async_remote_copy(
            src_ref=source,
            dst_ref=gots[level].at[stripe],
            send_sem=send_sem.at[stripe, level],
            recv_sem=recv_sem.at[stripe, level],
            device_id=(me + (1 << bit) * (1 - 2 * side(bit)),),
            device_id_type=MESH,
        )

    def step_on(stripe, level):
        which, lane, order = stripes[stripe]
        copy_of(stripe, level).wait_recv()
        if level == 0:
            for chunk in range(1 << (bits - 1)):
                held = parts[which][chunk, side(0), :, pl.ds(lane, 128)].astype(f32)
                total = held + gots[0][stripe, chunk].astype(f32)
                sums[0][stripe, placed(chunk, order)] = total.astype(bf16)
        else:
            bit = order[level - 1]
            half = 1 << (bits - 1 - level)
            held = sums[level - 1][stripe, pl.ds(side(bit) * half, half)].astype(f32)
            total = held + gots[level][stripe].astype(f32)
            if level < bits - 1:
                sums[level][stripe] = total.astype(bf16)
            else:
                outs[which][:, pl.ds(lane, 128)] = total[0]
        if level < bits - 1:
            copy_of(stripe, level + 1).start()

    moves = []
    for step in range(1, peers):
        peer = lax.rem(me + step, peers)
        for source, target, sent, landed in (
            (back_ref.at[peer], got_ref.at[me], row_send, row_recv),
            (stat_ref, stats_ref.at[me], stat_send, stat_recv),
        ):
            move = pltpu.make_async_remote_copy(
                src_ref=source,
                dst_ref=target,
                send_sem=sent.at[step],
                recv_sem=landed.at[step],
                device_id=(peer,),
                device_id_type=MESH,
            )
            move.start()
            moves.append(move)

    early = [s for s in range(len(stripes)) if stripes[s][0] == 0]
    late = [s for s in range(len(stripes)) if stripes[s][0] == 1]
    units = [late[k:k + 2] for k in range(0, len(late), 2)]
    for stripe in early:
        copy_of(stripe, 0).start()
    for stripe in early:
        step_on(stripe, 0)
    for move in moves:
        move.wait_recv()
    own.wait()
    back = got_ref[...].astype(f32).reshape(-1, width).astype(bf16)
    grad = local_ref[...] + jnp.dot(select_ref[...], back, preferred_element_type=f32)
    grad_ref[...] = jnp.where(pre_ref[...] > 0.0, grad, 0.0).astype(bf16)

    def products(unit):
        lane, span = stripes[unit[0]][1], 128 * len(unit)
        right = grad_ref[:, pl.ds(lane, span)]
        for r in range(relations):
            made = lax.dot_general(
                avg_ref[r], right, (((0,), (0,)), ((), ())), preferred_element_type=f32
            ).astype(bf16)
            low = r * width
            while low < (r + 1) * width:
                chunk, start = low // rows, low % rows
                size = min(rows - start, (r + 1) * width - low)
                piece = made[low - r * width:low - r * width + size]
                one_ref[chunk // 2, chunk % 2, pl.ds(start, size), pl.ds(lane, span)] = piece
                low += size
        for stripe in unit:
            copy_of(stripe, 0).start()

    done = 1
    for unit in units:
        for stripe in early:
            step_on(stripe, done)
        done += 1
        products(unit)
    for wave in range(bits + len(units) - 1):
        for k, unit in enumerate(units):
            if 0 <= wave - k < bits:
                for stripe in unit:
                    step_on(stripe, wave - k)
        if done < bits:
            for stripe in early:
                step_on(stripe, done)
            done += 1
    for level in range(bits):
        for stripe in range(len(stripes)):
            copy_of(stripe, level).wait_send()
    for move in moves:
        move.wait_send()


def tail(part_two, back, stat, local_grad, pre, select, avg_one, peers, slots):
    bits = peers.bit_length() - 1
    relations, nodes, width = avg_one.shape
    rows = part_two.shape[0] // peers
    orders = bit_orders(bits)
    stripes = []
    for which, columns in enumerate((part_two.shape[1], width)):
        for lane in range(0, columns, 128):
            stripes.append((which, lane, orders[len(stripes) % 2 if stripes else 2]))
    count = len(stripes)
    half = peers // 2
    stat = jnp.broadcast_to(stat.astype(f32), (1, 128))
    sums = [pltpu.VMEM((count, half >> k, rows, 128), bf16) for k in range(bits - 1)]
    gots = [pltpu.VMEM((count, half >> k, rows, 128), bf16) for k in range(bits)]
    grad_one, grad_two, stats = pl.pallas_call(
        functools.partial(tail_kernel, stripes, bits, relations),
        out_shape=[
            jax.ShapeDtypeStruct((rows, width), f32),
            jax.ShapeDtypeStruct((rows, part_two.shape[1]), f32),
            jax.ShapeDtypeStruct((peers, 1, 128), f32),
        ],
        in_specs=[pl.BlockSpec(memory_space=pltpu.VMEM)] * 7,
        out_specs=[pl.BlockSpec(memory_space=pltpu.VMEM)] * 3,
        scratch_shapes=[
            pltpu.VMEM((half, 2, rows, width), bf16),
            pltpu.VMEM((nodes, width), bf16),
            pltpu.VMEM((peers, slots, width), bf16),
        ] + sums + gots + [pltpu.SemaphoreType.DMA((count, bits))] * 2
        + [pltpu.SemaphoreType.DMA((peers,))] * 4 + [pltpu.SemaphoreType.DMA],
        compiler_params=pltpu.CompilerParams(
            collective_id=4, has_side_effects=True, vmem_limit_bytes=60 * 1024 * 1024
        ),
        name="tail",
    )(
        part_two.reshape(half, 2, rows, part_two.shape[1]),
        back.reshape(peers, slots, width),
        stat,
        local_grad,
        pre,
        select,
        avg_one,
    )
    return grad_one, grad_two, jnp.sum(stats[:, 0, 0])


def on_device(features, w_one, w_two, self_two, edge_src, edge_dst, send_rows, send_count, labels):
    peers = lax.axis_size("dom")
    node_rows, width = features.shape
    relations, blocks, edges = edge_src.shape
    slots = send_rows.shape[2]
    table_rows = node_rows + peers * slots
    labelled = labels >= 0
    local_count = jnp.sum(labelled.astype(f32))

    live = jnp.arange(slots, dtype=jnp.int32)[None, :] < send_count[0][:, None]
    picks = jnp.where(live, send_rows[0], -1).reshape(-1)
    select = (picks[:, None] == jnp.arange(node_rows, dtype=jnp.int32)[None, :]).astype(bf16)

    select_t = (picks[None, :] == jnp.arange(node_rows, dtype=jnp.int32)[:, None]).astype(bf16)

    arrived, label_count = exchange(jnp.dot(select, features), local_count, peers, slots, 1)
    hot_dst = edge_dst[:, :, None, :] == jnp.arange(128, dtype=jnp.int32)[None, None, :, None]
    hot_src = edge_src[:, :, None, :] == jnp.arange(table_rows, dtype=jnp.int32)[None, None, :, None]
    counts = jnp.einsum(
        "rbve,rbte->rbvt", hot_dst.astype(bf16), hot_src.astype(bf16), preferred_element_type=f32
    )
    adj = counts.astype(bf16).reshape(relations * blocks * 128, table_rows)
    norm = 1.0 / jnp.maximum(jnp.sum(hot_dst.astype(f32), axis=3), 1.0)
    norm = norm.reshape(relations * blocks * 128, 1)

    def averages(own, got):
        table = jnp.concatenate([own, got], axis=0)
        sums = jnp.dot(adj, table, preferred_element_type=f32)
        return (sums * norm).astype(bf16).reshape(relations, node_rows, width)

    avg_one = jnp.concatenate([averages(features, arrived), features[None]], axis=0)
    pre = jnp.einsum("rnd,rde->ne", avg_one, w_one, preferred_element_type=f32)
    hidden = jnp.maximum(pre, 0.0).astype(bf16)
    arrived_hidden, unused = exchange(jnp.dot(select, hidden), local_count, peers, slots, 2)
    avg_two = jnp.concatenate([averages(hidden, arrived_hidden), hidden[None]], axis=0)
    w_all = jnp.concatenate([w_two, self_two[None]], axis=0)
    logits = jnp.einsum("rnd,rdc->nc", avg_two, w_all, preferred_element_type=f32)

    classes = logits.shape[1]
    log_total = jax.nn.logsumexp(logits, axis=1)
    one_hot = (jnp.arange(classes, dtype=jnp.int32)[None, :] == labels[:, None]).astype(f32)
    picked = jnp.sum(logits * one_hot, axis=1)
    local_total = jnp.sum(jnp.where(labelled, log_total - picked, 0.0))
    softmax_out = jnp.exp(logits - log_total[:, None])
    grad_logits = (
        loss_scale * (softmax_out - one_hot) * labelled[:, None].astype(f32) / label_count
    ).astype(bf16)

    def products(left, right):
        full = jnp.einsum("rnd,nc->rdc", left, right, preferred_element_type=f32)
        return full.astype(bf16).reshape((relations + 1) * width, -1)

    padded = jnp.pad(grad_logits, ((0, 0), (0, -classes % 128)))
    part_two = products(avg_two, padded)
    spread = jnp.einsum("nc,rdc->rnd", grad_logits, w_two, preferred_element_type=f32)
    spread = (spread.reshape(-1, width) * norm).astype(bf16)
    table_grad = lax.dot_general(adj, spread, (((0,), (0,)), ((), ())), preferred_element_type=f32)
    local_grad = table_grad[:node_rows] + jnp.dot(
        grad_logits, self_two.T, preferred_element_type=f32
    )
    back = table_grad[node_rows:].astype(bf16)
    if (relations + 1) * width // peers % 16 == 0:
        grad_one, grad_two, total = tail(
            part_two, back, local_total, local_grad, pre, select_t, avg_one, peers, slots
        )
    else:
        returned, total = exchange(back, local_total, peers, slots, 3)
        grad_hidden = local_grad + jnp.dot(select_t, returned, preferred_element_type=f32)
        grad_pre = jnp.where(pre > 0.0, grad_hidden, 0.0).astype(bf16)
        grad_one, grad_two = scatter_sums(products(avg_one, grad_pre), part_two, peers)
    return (logits, total / label_count, grad_one, grad_two[:, :classes])


def solution(mesh):
    in_specs = (
        P("dom", None),
        P(),
        P(),
        P(),
        P(None, "dom", None),
        P(None, "dom", None),
        P("dom", None, None),
        P("dom", None),
        P("dom"),
    )
    out_specs = (P("dom", None), P(), P("dom", None), P("dom", None))
    return jax.shard_map(
        on_device, mesh=mesh, in_specs=in_specs, out_specs=out_specs, check_vma=False
    )
```

```python
import functools

import jax
import jax.numpy as jnp
from jax import lax
from jax.experimental import pallas as pl
from jax.experimental.pallas import tpu as pltpu
from jax.sharding import PartitionSpec as P

loss_scale = 256.0
f32 = jnp.float32
bf16 = jnp.bfloat16
MESH = pl.DeviceIdType.MESH


def build_counts(src_ref, dst_ref, adj_ref, norm_ref):
    relations, blocks, edges = src_ref.shape
    table_rows = adj_ref.shape[1]
    block_rows = lax.broadcasted_iota(jnp.int32, (128, edges), 0)
    sources = lax.broadcasted_iota(jnp.int32, (table_rows, edges), 0)
    for r in range(relations):
        for b in range(blocks):
            hot_dst = jnp.where(block_rows == dst_ref[r, pl.ds(b, 1), :], 1.0, 0.0)
            hot_src = jnp.where(sources == src_ref[r, pl.ds(b, 1), :], 1.0, 0.0).astype(bf16)
            counts = lax.dot_general(
                hot_dst.astype(bf16), hot_src, (((1,), (1,)), ((), ())), preferred_element_type=f32
            )
            spot = pl.ds((r * blocks + b) * 128, 128)
            adj_ref[spot, :] = counts.astype(bf16)
            norm_ref[spot, :] = 1.0 / jnp.maximum(jnp.sum(hot_dst, axis=1, keepdims=True), 1.0)


def first_kernel(peers, rows_ref, stat_ref, src_ref, dst_ref, got_ref, stats_ref, adj_ref, norm_ref, *sems):
    def beside():
        build_counts(src_ref, dst_ref, adj_ref, norm_ref)

    exchange_kernel(peers, rows_ref, stat_ref, got_ref, stats_ref, *sems, beside=beside)


def exchange_kernel(peers, rows_ref, stat_ref, got_ref, stats_ref, send_sem, recv_sem, stat_send, stat_recv, own_sem, beside=None):
    me = lax.axis_index("dom")
    barrier = pltpu.get_barrier_semaphore()
    for step in range(1, peers):
        peer = lax.rem(me + step, peers)
        pl.semaphore_signal(barrier, inc=1, device_id=(peer,), device_id_type=MESH)
    own = pltpu.make_async_copy(rows_ref.at[me], got_ref.at[me], own_sem)
    own.start()
    stats_ref[me] = stat_ref[...]
    pl.semaphore_wait(barrier, peers - 1)
    copies = []
    for step in range(1, peers):
        peer = lax.rem(me + step, peers)
        copies.append(
            pltpu.make_async_remote_copy(
                src_ref=rows_ref.at[peer],
                dst_ref=got_ref.at[me],
                send_sem=send_sem.at[step],
                recv_sem=recv_sem.at[step],
                device_id=(peer,),
                device_id_type=MESH,
            )
        )
        copies.append(
            pltpu.make_async_remote_copy(
                src_ref=stat_ref,
                dst_ref=stats_ref.at[me],
                send_sem=stat_send.at[step],
                recv_sem=stat_recv.at[step],
                device_id=(peer,),
                device_id_type=MESH,
            )
        )
        copies[-2].start()
        copies[-1].start()
    if beside is not None:
        beside()
    for copy in copies:
        copy.wait_recv()
    for copy in copies:
        copy.wait_send()
    own.wait()


def exchange(rows, stat, peers, slots, call, edge_pair=()):
    width = rows.shape[1]
    made = []
    if edge_pair:
        targets = edge_pair[0].shape[0] * edge_pair[0].shape[1] * 128
        table_rows = targets // edge_pair[0].shape[0] + peers * slots
        made = [
            jax.ShapeDtypeStruct((targets, table_rows), bf16),
            jax.ShapeDtypeStruct((targets, 1), f32),
        ]
    stat = jnp.broadcast_to(stat.astype(f32), (1, 128))
    got, stats, *made = pl.pallas_call(
        functools.partial(first_kernel if edge_pair else exchange_kernel, peers),
        out_shape=[
            jax.ShapeDtypeStruct((peers, slots, width), bf16),
            jax.ShapeDtypeStruct((peers, 1, 128), f32),
        ] + made,
        in_specs=[pl.BlockSpec(memory_space=pltpu.VMEM)] * (2 + len(edge_pair)),
        out_specs=[pl.BlockSpec(memory_space=pltpu.VMEM)] * (2 + len(made)),
        scratch_shapes=[pltpu.SemaphoreType.DMA((peers,))] * 4 + [pltpu.SemaphoreType.DMA],
        compiler_params=pltpu.CompilerParams(
            collective_id=call, has_side_effects=True, vmem_limit_bytes=(32 if edge_pair else 8) * 1024 * 1024
        ),
        name=f"exchange_{call}",
    )(rows.reshape(peers, slots, width), stat, *edge_pair)
    return (got.reshape(peers * slots, width), jnp.sum(stats[:, 0, 0]), *made)


def bit_orders(bits):
    links = list(range(1, bits))
    swapped = links[1::-1] + links[2:]
    return links, swapped, links[2:] + links[:2]


def placed(chunk, order):
    spot = 0
    for bit in order:
        spot = spot * 2 + ((chunk >> (bit - 1)) & 1)
    return spot


def scatter_kernel(stripes, bits, *refs):
    count = len(stripes)
    parts, outs, rest = refs[:2], refs[2:4], refs[4:]
    sums, gots, send_sem, recv_sem = rest[:bits - 1], rest[bits - 1:2 * bits - 1], rest[-2], rest[-1]
    me = lax.axis_index("dom")
    barrier = pltpu.get_barrier_semaphore()

    def side(bit):
        return lax.rem(me // (1 << bit), 2)

    def partner(bit):
        return me + (1 << bit) * (1 - 2 * side(bit))

    for bit in range(bits):
        pl.semaphore_signal(barrier, inc=1, device_id=(partner(bit),), device_id_type=MESH)
    pl.semaphore_wait(barrier, bits)

    def copy_of(stripe, level):
        which, lane, order = stripes[stripe]
        if level == 0:
            bit = 0
            source = parts[which].at[:, 1 - side(0), :, pl.ds(lane, 128)]
        else:
            bit = order[level - 1]
            half = 1 << (bits - 1 - level)
            source = sums[level - 1].at[stripe, pl.ds((1 - side(bit)) * half, half)]
        return pltpu.make_async_remote_copy(
            src_ref=source,
            dst_ref=gots[level].at[stripe],
            send_sem=send_sem.at[stripe, level],
            recv_sem=recv_sem.at[stripe, level],
            device_id=(partner(bit),),
            device_id_type=MESH,
        )

    def add_up(stripe, level):
        which, lane, order = stripes[stripe]
        if level == 0:
            for chunk in range(1 << (bits - 1)):
                own = parts[which][chunk, side(0), :, pl.ds(lane, 128)].astype(f32)
                total = own + gots[0][stripe, chunk].astype(f32)
                sums[0][stripe, placed(chunk, order)] = total.astype(bf16)
            return
        bit = order[level - 1]
        half = 1 << (bits - 1 - level)
        own = sums[level - 1][stripe, pl.ds(side(bit) * half, half)].astype(f32)
        total = own + gots[level][stripe].astype(f32)
        if level < bits - 1:
            sums[level][stripe] = total.astype(bf16)
        else:
            outs[which][:, pl.ds(lane, 128)] = total[0]

    for stripe in range(count):
        copy_of(stripe, 0).start()
    units = [list(range(0, 3))] + [list(range(k, min(k + 2, count))) for k in range(3, count, 2)]
    for wave in range(len(units) + bits - 1):
        for level in range(bits):
            for stripe in units[wave - level] if 0 <= wave - level < len(units) else ():
                copy_of(stripe, level).wait_recv()
                add_up(stripe, level)
                if level < bits - 1:
                    copy_of(stripe, level + 1).start()
    for level in range(bits):
        for stripe in range(count):
            copy_of(stripe, level).wait_send()


def scatter_sums(first, second, peers):
    bits = peers.bit_length() - 1
    rows = first.shape[0] // peers
    orders = bit_orders(bits)
    stripes = []
    for which, part in enumerate((first, second)):
        for lane in range(0, part.shape[1], 128):
            stripes.append((which, lane, orders[len(stripes) % 2 if stripes else 2]))
    count = len(stripes)
    half = peers // 2
    sums = [pltpu.VMEM((count, half >> k, rows, 128), bf16) for k in range(bits - 1)]
    gots = [pltpu.VMEM((count, half >> k, rows, 128), bf16) for k in range(bits)]
    views = [part.reshape(half, 2, rows, part.shape[1]) for part in (first, second)]
    return pl.pallas_call(
        functools.partial(scatter_kernel, stripes, bits),
        out_shape=[jax.ShapeDtypeStruct((rows, part.shape[1]), f32) for part in (first, second)],
        in_specs=[pl.BlockSpec(memory_space=pltpu.VMEM)] * 2,
        out_specs=[pl.BlockSpec(memory_space=pltpu.VMEM)] * 2,
        scratch_shapes=sums + gots + [
            pltpu.SemaphoreType.DMA((count, bits)),
            pltpu.SemaphoreType.DMA((count, bits)),
        ],
        compiler_params=pltpu.CompilerParams(
            collective_id=0, has_side_effects=True, vmem_limit_bytes=60 * 1024 * 1024
        ),
        name="scatter_sums",
    )(*views)


def tail_kernel(
    stripes, bits, relations,
    two_ref, back_ref, stat_ref, local_ref, pre_ref, select_ref, avg_ref,
    one_out, two_out, stats_ref, one_ref, grad_ref, got_ref, *rest
):
    peers = 1 << bits
    sums, gots = rest[:bits - 1], rest[bits - 1:2 * bits - 1]
    send_sem, recv_sem, row_send, row_recv, stat_send, stat_recv, own_sem = rest[2 * bits - 1:]
    parts, outs = (two_ref, one_ref), (two_out, one_out)
    rows, width = one_ref.shape[2:]
    me = lax.axis_index("dom")
    barrier = pltpu.get_barrier_semaphore()
    for step in range(1, peers):
        peer = lax.rem(me + step, peers)
        pl.semaphore_signal(barrier, inc=1, device_id=(peer,), device_id_type=MESH)
    own = pltpu.make_async_copy(back_ref.at[me], got_ref.at[me], own_sem)
    own.start()
    stats_ref[me] = stat_ref[...]
    pl.semaphore_wait(barrier, peers - 1)

    def side(bit):
        return lax.rem(me // (1 << bit), 2)

    def copy_of(stripe, level):
        which, lane, order = stripes[stripe]
        if level == 0:
            bit = 0
            source = parts[which].at[:, 1 - side(0), :, pl.ds(lane, 128)]
        else:
            bit = order[level - 1]
            half = 1 << (bits - 1 - level)
            source = sums[level - 1].at[stripe, pl.ds((1 - side(bit)) * half, half)]
        return pltpu.make_async_remote_copy(
            src_ref=source,
            dst_ref=gots[level].at[stripe],
            send_sem=send_sem.at[stripe, level],
            recv_sem=recv_sem.at[stripe, level],
            device_id=(me + (1 << bit) * (1 - 2 * side(bit)),),
            device_id_type=MESH,
        )

    def step_on(stripe, level):
        which, lane, order = stripes[stripe]
        copy_of(stripe, level).wait_recv()
        if level == 0:
            for chunk in range(1 << (bits - 1)):
                held = parts[which][chunk, side(0), :, pl.ds(lane, 128)].astype(f32)
                total = held + gots[0][stripe, chunk].astype(f32)
                sums[0][stripe, placed(chunk, order)] = total.astype(bf16)
        else:
            bit = order[level - 1]
            half = 1 << (bits - 1 - level)
            held = sums[level - 1][stripe, pl.ds(side(bit) * half, half)].astype(f32)
            total = held + gots[level][stripe].astype(f32)
            if level < bits - 1:
                sums[level][stripe] = total.astype(bf16)
            else:
                outs[which][:, pl.ds(lane, 128)] = total[0]
        if level < bits - 1:
            copy_of(stripe, level + 1).start()

    moves = []
    for step in range(1, peers):
        peer = lax.rem(me + step, peers)
        for source, target, sent, landed in (
            (back_ref.at[peer], got_ref.at[me], row_send, row_recv),
            (stat_ref, stats_ref.at[me], stat_send, stat_recv),
        ):
            move = pltpu.make_async_remote_copy(
                src_ref=source,
                dst_ref=target,
                send_sem=sent.at[step],
                recv_sem=landed.at[step],
                device_id=(peer,),
                device_id_type=MESH,
            )
            move.start()
            moves.append(move)

    early = [s for s in range(len(stripes)) if stripes[s][0] == 0]
    late = [s for s in range(len(stripes)) if stripes[s][0] == 1]
    units = [late[k:k + 2] for k in range(0, len(late), 2)]
    for stripe in early:
        copy_of(stripe, 0).start()
    for stripe in early:
        step_on(stripe, 0)
    for move in moves:
        move.wait_recv()
    own.wait()
    back = got_ref[...].astype(f32).reshape(-1, width).astype(bf16)
    grad = local_ref[...] + jnp.dot(select_ref[...], back, preferred_element_type=f32)
    grad_ref[...] = jnp.where(pre_ref[...] > 0.0, grad, 0.0).astype(bf16)

    def products(unit):
        lane, span = stripes[unit[0]][1], 128 * len(unit)
        right = grad_ref[:, pl.ds(lane, span)]
        for r in range(relations):
            made = lax.dot_general(
                avg_ref[r], right, (((0,), (0,)), ((), ())), preferred_element_type=f32
            ).astype(bf16)
            low = r * width
            while low < (r + 1) * width:
                chunk, start = low // rows, low % rows
                size = min(rows - start, (r + 1) * width - low)
                piece = made[low - r * width:low - r * width + size]
                one_ref[chunk // 2, chunk % 2, pl.ds(start, size), pl.ds(lane, span)] = piece
                low += size
        for stripe in unit:
            copy_of(stripe, 0).start()

    done = 1
    for unit in units:
        for stripe in early:
            step_on(stripe, done)
        done += 1
        products(unit)
    for wave in range(bits + len(units) - 1):
        for k, unit in enumerate(units):
            if 0 <= wave - k < bits:
                for stripe in unit:
                    step_on(stripe, wave - k)
        if done < bits:
            for stripe in early:
                step_on(stripe, done)
            done += 1
    for level in range(bits):
        for stripe in range(len(stripes)):
            copy_of(stripe, level).wait_send()
    for move in moves:
        move.wait_send()


def tail(part_two, back, stat, local_grad, pre, select, avg_one, peers, slots):
    bits = peers.bit_length() - 1
    relations, nodes, width = avg_one.shape
    rows = part_two.shape[0] // peers
    orders = bit_orders(bits)
    stripes = []
    for which, columns in enumerate((part_two.shape[1], width)):
        for lane in range(0, columns, 128):
            stripes.append((which, lane, orders[len(stripes) % 2 if stripes else 2]))
    count = len(stripes)
    half = peers // 2
    stat = jnp.broadcast_to(stat.astype(f32), (1, 128))
    sums = [pltpu.VMEM((count, half >> k, rows, 128), bf16) for k in range(bits - 1)]
    gots = [pltpu.VMEM((count, half >> k, rows, 128), bf16) for k in range(bits)]
    grad_one, grad_two, stats = pl.pallas_call(
        functools.partial(tail_kernel, stripes, bits, relations),
        out_shape=[
            jax.ShapeDtypeStruct((rows, width), f32),
            jax.ShapeDtypeStruct((rows, part_two.shape[1]), f32),
            jax.ShapeDtypeStruct((peers, 1, 128), f32),
        ],
        in_specs=[pl.BlockSpec(memory_space=pltpu.VMEM)] * 7,
        out_specs=[pl.BlockSpec(memory_space=pltpu.VMEM)] * 3,
        scratch_shapes=[
            pltpu.VMEM((half, 2, rows, width), bf16),
            pltpu.VMEM((nodes, width), bf16),
            pltpu.VMEM((peers, slots, width), bf16),
        ] + sums + gots + [pltpu.SemaphoreType.DMA((count, bits))] * 2
        + [pltpu.SemaphoreType.DMA((peers,))] * 4 + [pltpu.SemaphoreType.DMA],
        compiler_params=pltpu.CompilerParams(
            collective_id=4, has_side_effects=True, vmem_limit_bytes=60 * 1024 * 1024
        ),
        name="tail",
    )(
        part_two.reshape(half, 2, rows, part_two.shape[1]),
        back.reshape(peers, slots, width),
        stat,
        local_grad,
        pre,
        select,
        avg_one,
    )
    return grad_one, grad_two, jnp.sum(stats[:, 0, 0])


def on_device(features, w_one, w_two, self_two, edge_src, edge_dst, send_rows, send_count, labels):
    peers = lax.axis_size("dom")
    node_rows, width = features.shape
    relations, blocks, edges = edge_src.shape
    slots = send_rows.shape[2]
    table_rows = node_rows + peers * slots
    labelled = labels >= 0
    local_count = jnp.sum(labelled.astype(f32))

    live = jnp.arange(slots, dtype=jnp.int32)[None, :] < send_count[0][:, None]
    picks = jnp.where(live, send_rows[0], -1).reshape(-1)
    select = (picks[:, None] == jnp.arange(node_rows, dtype=jnp.int32)[None, :]).astype(bf16)

    select_t = (picks[None, :] == jnp.arange(node_rows, dtype=jnp.int32)[:, None]).astype(bf16)

    arrived, label_count, adj, norm = exchange(
        jnp.dot(select, features), local_count, peers, slots, 1, (edge_src, edge_dst)
    )
    def averages(own, got):
        table = jnp.concatenate([own, got], axis=0)
        sums = jnp.dot(adj, table, preferred_element_type=f32)
        return (sums * norm).astype(bf16).reshape(relations, node_rows, width)

    avg_one = jnp.concatenate([averages(features, arrived), features[None]], axis=0)
    pre = jnp.einsum("rnd,rde->ne", avg_one, w_one, preferred_element_type=f32)
    hidden = jnp.maximum(pre, 0.0).astype(bf16)
    arrived_hidden, unused = exchange(jnp.dot(select, hidden), local_count, peers, slots, 2)
    avg_two = jnp.concatenate([averages(hidden, arrived_hidden), hidden[None]], axis=0)
    w_all = jnp.concatenate([w_two, self_two[None]], axis=0)
    logits = jnp.einsum("rnd,rdc->nc", avg_two, w_all, preferred_element_type=f32)

    classes = logits.shape[1]
    log_total = jax.nn.logsumexp(logits, axis=1)
    one_hot = (jnp.arange(classes, dtype=jnp.int32)[None, :] == labels[:, None]).astype(f32)
    picked = jnp.sum(logits * one_hot, axis=1)
    local_total = jnp.sum(jnp.where(labelled, log_total - picked, 0.0))
    softmax_out = jnp.exp(logits - log_total[:, None])
    grad_logits = (
        loss_scale * (softmax_out - one_hot) * labelled[:, None].astype(f32) / label_count
    ).astype(bf16)

    def products(left, right):
        full = jnp.einsum("rnd,nc->rdc", left, right, preferred_element_type=f32)
        return full.astype(bf16).reshape((relations + 1) * width, -1)

    padded = jnp.pad(grad_logits, ((0, 0), (0, -classes % 128)))
    part_two = products(avg_two, padded)
    spread = jnp.einsum("nc,rdc->rnd", grad_logits, w_two, preferred_element_type=f32)
    spread = (spread.reshape(-1, width) * norm).astype(bf16)
    table_grad = lax.dot_general(adj, spread, (((0,), (0,)), ((), ())), preferred_element_type=f32)
    local_grad = table_grad[:node_rows] + jnp.dot(
        grad_logits, self_two.T, preferred_element_type=f32
    )
    back = table_grad[node_rows:].astype(bf16)
    if (relations + 1) * width // peers % 16 == 0:
        grad_one, grad_two, total = tail(
            part_two, back, local_total, local_grad, pre, select_t, avg_one, peers, slots
        )
    else:
        returned, total = exchange(back, local_total, peers, slots, 3)
        grad_hidden = local_grad + jnp.dot(select_t, returned, preferred_element_type=f32)
        grad_pre = jnp.where(pre > 0.0, grad_hidden, 0.0).astype(bf16)
        grad_one, grad_two = scatter_sums(products(avg_one, grad_pre), part_two, peers)
    return (logits, total / label_count, grad_one, grad_two[:, :classes])


def solution(mesh):
    in_specs = (
        P("dom", None),
        P(),
        P(),
        P(),
        P(None, "dom", None),
        P(None, "dom", None),
        P("dom", None, None),
        P("dom", None),
        P("dom"),
    )
    out_specs = (P("dom", None), P(), P("dom", None), P("dom", None))
    return jax.shard_map(
        on_device, mesh=mesh, in_specs=in_specs, out_specs=out_specs, check_vma=False
    )
```
